256 devices in a mesh: replica: 16 (over z, core), model: 4 (over x), copy: 4 (over y).
Axes of the slice: x: 4, y: 4, z: 8, core: 2. Of those that a mesh axis runs over, the one named last changes fastest.
Arguments:
- slope_up: bfloat16 [64, 1280, 5120], P(('copy', 'replica'), None, 'model'), parts along dimension 0, may hold values from -0.875 to 0.875
- slope_down: bfloat16 [64, 5120, 1280], P(('copy', 'replica'), 'model'), parts along dimension 0, may hold values from -0.875 to 0.875
- slope_norm: bfloat16 [64, 1280], P(('copy', 'replica')), parts along dimension 0, may hold values from -8 to 8
- param_up: float32 [5120, 5120], P(('copy', 'replica'), 'model'), parts along dimension 0, may hold values from -0.25 to 0.25
- param_down: float32 [20480, 1280], P(('copy', 'model'), 'replica'), parts along dimension 0, may hold values from -0.125 to 0.125
- param_norm: float32 [5120], P(('copy', 'replica')), parts along dimension 0, may hold values from 0.25 to 1.75
Outputs:
- half_up: bfloat16 [5120, 5120], P('copy', 'model'), parts along dimension 0
- half_down: bfloat16 [20480, 1280], P(('copy', 'model')), parts along dimension 0
- half_norm: bfloat16 [5120], P('copy'), parts along dimension 0
- next_up: float32 [5120, 5120], P(('copy', 'replica'), 'model'), parts along dimension 0
- next_down: float32 [20480, 1280], P(('copy', 'model'), 'replica'), parts along dimension 0
- next_norm: float32 [5120], P(('copy', 'replica')), parts along dimension 0
The draws below stay inside these ranges and needn't reach their ends.
There are 4 independent parts, one for each index of `copy`. The reference program is written for one: setup_inputs(seed, part) draws one part's arguments, and reference() takes and returns one part's arrays. A program takes and returns all parts, laid end to end along the dimension named above; each array names one. Nothing has to cross between parts.
All inputs are finite; a program needn't handle non-finite values.
Results may differ from the reference program's by a relative error of at most 0.011.
Values may be sent and summed in bfloat16 or wider, within the bound.
A program may use at most 128 MiB of HBM per device.

```python
import jax
import jax.numpy as jnp
from jax import lax

WIDTH = 1280
INNER = 5120
REPLICAS = 16


def spiked(drawn, rng, source, target, shards_of, factor):
    def block_of(dim):
        return (jnp.arange(drawn.shape[dim]) // (drawn.shape[dim] // shards_of)).reshape((-1,) + (1,) * (drawn.ndim - 1 - dim))

    first = jax.random.permutation(rng, shards_of)[block_of(target)]
    other_side = (block_of(target) + shards_of // 2) % shards_of
    return jnp.where((block_of(source) == first) | (block_of(source) == other_side), factor * drawn, drawn)


def level_of(stream_key, shape, cuts, least, top_value):
    level = 1.0
    for dim, parts in cuts:
        steps = jax.random.uniform(jax.random.fold_in(jax.random.fold_in(stream_key, 6), dim), (parts,), jnp.float32, least / len(cuts), top_value / len(cuts))
        level = level * jnp.repeat(jnp.exp(steps), shape[dim] // parts).reshape((-1,) + (1,) * (len(shape) - 1 - dim))
    return level


def noise_with(own_key, dims, spread, limit, pieces, heavy, dtype=jnp.bfloat16):
    array = spread * jax.random.normal(own_key, dims, jnp.float32)
    if pieces:
        array = array * level_of(own_key, dims, pieces, -0.22, 0.18)
    return jnp.clip(spiked(array, jax.random.fold_in(own_key, 3), *heavy), -limit, limit).astype(dtype)


def setup_inputs(seed: int = 0, part: int = 0) -> dict:
    key_of = jax.random.split(jax.random.key(seed), 7)
    part_keys = jax.random.split(jax.random.fold_in(key_of[6], part), 7)
    return {
        "slope_up": noise_with(part_keys[0], (REPLICAS, WIDTH, INNER), 0.1, 0.875, ((0, 16), (2, 4)), (0, 1, 16, 2.0)),
        "slope_down": noise_with(part_keys[1], (REPLICAS, INNER, WIDTH), 0.1, 0.875, ((0, 16), (1, 4)), (0, 2, 16, 2.0)),
        "slope_norm": noise_with(part_keys[2], (REPLICAS, WIDTH), 1.0, 8.0, ((0, 16),), (0, 1, 16, 2.0)),
        "param_up": noise_with(part_keys[3], (WIDTH, INNER), WIDTH ** -0.5, 0.25, ((0, 16), (1, 4)), (1, 0, 16, 2.0), jnp.float32),
        "param_down": noise_with(part_keys[4], (INNER, WIDTH), INNER ** -0.5, 0.125, ((0, 4), (1, 16)), (0, 1, 16, 2.0), jnp.float32),
        "param_norm": jnp.clip(1.0 + 0.15 * jax.random.normal(part_keys[5], (WIDTH,), jnp.float32), 0.25, 1.75),
    }


learn_rate = 0.5

def reference(slope_up, slope_down, slope_norm, param_up, param_down, param_norm):
    mean_up = lax.optimization_barrier(jnp.sum(slope_up.astype(jnp.float32), axis=0)) * REPLICAS ** (-0.5)
    mean_down = lax.optimization_barrier(jnp.sum(slope_down.astype(jnp.float32), axis=0)) * REPLICAS ** (-0.5)
    mean_norm = lax.optimization_barrier(jnp.sum(slope_norm.astype(jnp.float32), axis=0)) * REPLICAS ** (-0.5)
    ratio_up = jnp.sqrt(lax.optimization_barrier(jnp.sum(param_up * param_up, axis=1, keepdims=True))) * lax.rsqrt(lax.optimization_barrier(jnp.sum(mean_up * mean_up, axis=1, keepdims=True)) + 1e-06)
    mean_up = mean_up * ratio_up
    ratio_down = jnp.sqrt(lax.optimization_barrier(jnp.sum(param_down * param_down, axis=0, keepdims=True))) * lax.rsqrt(lax.optimization_barrier(jnp.sum(mean_down * mean_down, axis=0, keepdims=True)) + 1e-06)
    mean_down = mean_down * ratio_down
    next_up = param_up - learn_rate * mean_up
    next_down = param_down - learn_rate * mean_down
    next_norm = param_norm - learn_rate * mean_norm
    half_up = next_up.astype(jnp.bfloat16)
    half_down = next_down.astype(jnp.bfloat16)
    half_norm = next_norm.astype(jnp.bfloat16)
    return (half_up, half_down, half_norm, next_up, next_down, next_norm)
```

```python
import functools

import jax
import jax.numpy as jnp
from jax import lax
from jax.experimental import pallas as pl
from jax.experimental.pallas import tpu as pltpu
from jax.sharding import PartitionSpec as P

learn_rate = 0.5
eps = 1e-06
MESH = pl.DeviceIdType.MESH
UP, DOWN = 0, 1


def kernel(
    size,
    chips,
    models,
    up_hbm,
    down_hbm,
    row_in,
    param_up_hbm,
    param_down_hbm,
    half_up,
    half_down,
    next_up,
    next_down,
    half_norm,
    next_norm,
    own_up,
    raw_down,
    own_down,
    pair_in,
    send_buf,
    recv_buf,
    gathered,
    param,
    mean,
    sizes,
    sizes_in,
    rows,
    load_sem,
    pair_send,
    pair_recv,
    rs_send,
    rs_recv,
    ag_send,
    ag_recv,
    fwd_send,
    fwd_recv,
    size_send,
    size_recv,
    row_send,
    row_recv,
):
    f32, bf16 = jnp.float32, jnp.bfloat16
    share = size // (2 * chips)
    cols = size // 2
    replica = lax.axis_index("replica")
    model = lax.axis_index("model")
    z, c = replica // 2, replica % 2
    partner = {"replica": z * 2 + (1 - c)}
    rate = (2 * chips) ** (-0.5)

    def chip_at(offset):
        return lax.rem(z + offset + 2 * chips, chips)

    def neighbour(d):
        return {"replica": chip_at(1 if d == 0 else -1) * 2 + c}

    def rows_of(chip, core):
        return pl.ds(pl.multiple_of((chip * 2 + core) * share, 16), share)

    def half_cols(h):
        return pl.ds(h * cols, cols)

    def rdma(src, dst, send, recv, device):
        return pltpu.make_async_remote_copy(
            src_ref=src, dst_ref=dst, send_sem=send, recv_sem=recv, device_id=device, device_id_type=MESH
        )

    pending = []
    own = (own_up, own_down)
    full = (half_up, gathered)
    order = (4, 3, -3, 2, -2, 1, -1, 0)

    up_loads = {}
    for i, o in enumerate(order):
        at = rows_of(chip_at(o), c)
        up_loads[o] = pltpu.make_async_copy(up_hbm.at[at, :], own_up.at[at, :], load_sem.at[i])
        up_loads[o].start()
    down_load = pltpu.make_async_copy(down_hbm, raw_down, load_sem.at[8])
    down_load.start()
    param_loads = [
        pltpu.make_async_copy(param_up_hbm, param.at[UP], load_sem.at[9]),
        pltpu.make_async_copy(param_down_hbm, param.at[DOWN], load_sem.at[10]),
    ]
    for load in param_loads:
        load.start()

    barrier = pltpu.get_barrier_semaphore()
    others = [partner, neighbour(0), neighbour(1)]
    others += [{"model": lax.rem(model + d, models)} for d in range(1, models)]
    for device in others:
        pl.semaphore_signal(barrier, inc=1, device_id=device, device_id_type=MESH)
    pl.semaphore_wait(barrier, len(others))

    def pair_copy(p, o, core):
        at = rows_of(chip_at(o), core)
        src = up_hbm if p == UP else own_down
        i = order.index(o)
        return rdma(src.at[at, :], pair_in.at[p, o % chips], pair_send.at[p, i], pair_recv.at[p, i], partner)

    def start_pairs(p):
        for o in order:
            copy = pair_copy(p, o, 1 - c)
            copy.start()
            pending.append(copy)

    ready = set()

    def pair_sum(p, o, h):
        if (p, o) not in ready:
            ready.add((p, o))
            if p == UP:
                up_loads[o].wait()
            pair_copy(p, o, c).wait_recv()
        mine = own[p][rows_of(chip_at(o), c), half_cols(h)]
        return mine.astype(f32) + pair_in[p, o % chips, :, half_cols(h)].astype(f32)

    def rs_index(d, k, h):
        return 0 if k == 0 else 2 * k - 1 + (h != d)

    def rs_copy(p, d, k, h):
        i = rs_index(d, k, h)
        return rdma(send_buf.at[p, d, i], recv_buf.at[p, d, i], rs_send.at[p, d, i], rs_recv.at[p, d, i], neighbour(d))

    def rs_step(p, k, long_half):
        for d in range(2):
            h = d if long_half else 1 - d
            value = pair_sum(p, (4 - k if d == 0 else k - 4) if k else 4, h)
            if k >= 2 or (k == 1 and long_half):
                rs_copy(p, d, k - 1, h).wait_recv()
                value = value + recv_buf[p, d, rs_index(d, k - 1, h)].astype(f32)
            send_buf[p, d, rs_index(d, k, h)] = value.astype(bf16)
            copy = rs_copy(p, d, k, h)
            copy.start()
            pending.append(copy)

    def size_copy(p, e):
        return rdma(
            sizes.at[p],
            sizes_in.at[p, e - 1],
            size_send.at[p, e - 1],
            size_recv.at[p, e - 1],
            {"model": lax.rem(model + e, models)},
        )

    def finish_sum(p):
        total = jnp.zeros((share, 1), f32)
        for h in range(2):
            for d in range(2):
                rs_copy(p, d, 3, h).wait_recv()
            value = pair_sum(p, 0, h)
            for d in range(2):
                value = value + recv_buf[p, d, rs_index(d, 3, h)].astype(f32)
            value = value * rate
            mean[p, :, half_cols(h)] = value
            total = total + jnp.sum(value * value, axis=1, keepdims=True)
        param_loads[p].wait()
        weights = jnp.sum(param[p] * param[p], axis=1, keepdims=True)
        lane = lax.broadcasted_iota(jnp.int32, (share, 128), 1)
        sizes[p] = jnp.where(lane < 64, total, weights)
        for e in range(1, models):
            copy = size_copy(p, e)
            copy.start()
            pending.append(copy)

    def update(p):
        both = sizes[p]
        for e in range(1, models):
            size_copy(p, e).wait_recv()
            both = both + sizes_in[p, e - 1]
        ratio = jnp.sqrt(both[:, 64:65]) * lax.rsqrt(both[:, 0:1] + eps)
        value = param[p] - learn_rate * (mean[p] * ratio)
        out = next_up if p == UP else next_down
        out[...] = value
        full[p][rows_of(z, c), :] = value.astype(bf16)
        copy = rdma(
            full[p].at[rows_of(z, c), :], full[p].at[rows_of(z, c), :], fwd_send.at[p, 14], fwd_recv.at[p, 14], partner
        )
        copy.start()
        pending.append(copy)

    def ag_index(d, k, h):
        return 2 * k + (h != d)

    def ag_copy(p, d, k, h, hop):
        chip = chip_at((-k - hop) if d == 0 else (k + hop))
        at = full[p].at[rows_of(chip, c), half_cols(h)]
        i = ag_index(d, k, h)
        return rdma(at, at, ag_send.at[p, d, i], ag_recv.at[p, d, i], neighbour(d))

    def forward_copy(p, d, k, h, core):
        chip = chip_at((-k - 1) if d == 0 else (k + 1))
        at = full[p].at[rows_of(chip, core), half_cols(h)]
        i = d * 7 + ag_index(d, k, h)
        return rdma(at, at, fwd_send.at[p, i], fwd_recv.at[p, i], partner)

    def ag_arrive(p, k, long_half):
        for d in range(2):
            h = d if long_half else 1 - d
            ag_copy(p, d, k, h, 1).wait_recv()
            copy = forward_copy(p, d, k, h, c)
            copy.start()
            pending.append(copy)

    def ag_step(p, k, long_half):
        for d in range(2):
            h = d if long_half else 1 - d
            if k:
                ag_copy(p, d, k - 1, h, 1).wait_recv()
            copy = ag_copy(p, d, k, h, 0)
            copy.start()
            pending.append(copy)
            if k:
                copy = forward_copy(p, d, k - 1, h, c)
                copy.start()
                pending.append(copy)

    def forwarded(p, k, long_half):
        for d in range(2):
            h = d if long_half else 1 - d
            forward_copy(p, d, k, h, 1 - c).wait_recv()

    def row_copy(d, k, hop):
        chip = chip_at((-k - hop) if d == 0 else (k + hop))
        at = rows.at[c, chip]
        return rdma(at, at, row_send.at[d, k], row_recv.at[d, k], neighbour(d))

    def row_step(k):
        for d in range(2):
            if k:
                if d == 1 and k == 4:
                    continue
                row_copy(d, k - 1, 1).wait_recv()
            if k < 4 - d:
                copy = row_copy(d, k, 0)
                copy.start()
                pending.append(copy)

    def row_pair(core):
        return rdma(rows.at[core], rows.at[core], row_send.at[0, 4], row_recv.at[0, 4], partner)

    def finish_rows():
        row_pair(1 - c).wait_recv()
        total = jnp.zeros((1, size), f32)
        gains = jnp.zeros((8, size), f32)
        wide = lax.broadcasted_iota(jnp.int32, (8, size), 1)
        for chip in range(chips):
            for core in range(2):
                total = total + rows[core, chip, :, :size]
                piece = jnp.broadcast_to(rows[core, chip, :, size:], (8, 128))
                piece = jnp.concatenate([piece] + [jnp.zeros((8, 128), f32)] * (size // 128 - 1), axis=1)
                start = (chip * 2 + core) * share
                moved = pltpu.roll(piece, start, 1) if start else piece
                gains = jnp.where((wide >= start) & (wide < start + share), moved, gains)
        gains = gains - learn_rate * (jnp.broadcast_to(total, (8, size)) * rate)
        half_norm[...] = gains[0:1].astype(bf16)
        shift = lax.rem(size - replica * share, size)
        next_norm[...] = pltpu.roll(gains, shift, 1)[0:1, 0:128]

    def turn_in(lo, hi):
        @pl.loop(lo, hi)
        def _(i):
            at = pl.ds(pl.multiple_of(i * 128, 128), 128)
            own_down[at, :] = raw_down[:, at].T

    low = (5 * chip_at(4)) // 4

    def turn_out(lo, hi):
        @pl.loop(lo, hi)
        def _(i):
            j = lax.rem(low + i, size // 128)
            at = pl.ds(pl.multiple_of(j * 128, 128), 128)
            half_down[:, at] = gathered[at, :].T

    L, S = True, False
    start_pairs(UP)
    rows[c, z] = row_in[...]
    rs_step(UP, 0, L)
    rs_step(UP, 1, S)
    row_step(0)
    down_load.wait()
    turn_in(0, size // 128)
    start_pairs(DOWN)
    rs_step(UP, 1, L)
    rs_step(UP, 2, S)
    row_step(1)
    rs_step(UP, 2, L)
    rs_step(UP, 3, S)
    row_step(2)
    rs_step(DOWN, 0, L)
    rs_step(UP, 3, L)
    rs_step(DOWN, 1, S)
    row_step(3)
    rs_step(DOWN, 1, L)
    finish_sum(UP)
    rs_step(DOWN, 2, S)
    rs_step(DOWN, 2, L)
    update(UP)
    rs_step(DOWN, 3, S)
    ag_step(UP, 0, L)
    rs_step(DOWN, 3, L)
    ag_step(UP, 0, S)
    row_step(4)
    copy = row_pair(c)
    copy.start()
    pending.append(copy)
    ag_step(UP, 1, L)
    finish_sum(DOWN)
    ag_step(UP, 1, S)
    ag_step(UP, 2, L)
    update(DOWN)
    ag_step(UP, 2, S)
    ag_step(DOWN, 0, L)
    ag_step(UP, 3, L)
    ag_step(DOWN, 0, S)
    ag_arrive(UP, 2, S)
    ag_step(DOWN, 1, L)
    ag_arrive(UP, 3, L)
    ag_step(DOWN, 1, S)
    finish_rows()
    ag_step(DOWN, 2, L)
    ag_step(DOWN, 2, S)
    rdma(
        full[DOWN].at[rows_of(z, 1 - c), :], full[DOWN].at[rows_of(z, 1 - c), :], fwd_send.at[DOWN, 14], fwd_recv.at[DOWN, 14], partner
    ).wait_recv()
    forwarded(DOWN, 0, L)
    forwarded(DOWN, 0, S)
    turn_out(5, 7)
    ag_step(DOWN, 3, L)
    forwarded(DOWN, 1, L)
    forwarded(DOWN, 1, S)
    turn_out(4, 5)
    turn_out(7, 8)
    ag_arrive(DOWN, 2, S)
    forwarded(DOWN, 2, L)
    forwarded(DOWN, 2, S)
    turn_out(2, 4)
    turn_out(8, 10)
    ag_arrive(DOWN, 3, L)
    rdma(
        full[UP].at[rows_of(z, 1 - c), :], full[UP].at[rows_of(z, 1 - c), :], fwd_send.at[UP, 14], fwd_recv.at[UP, 14], partner
    ).wait_recv()
    for k in range(3):
        forwarded(UP, k, L)
        forwarded(UP, k, S)
    forwarded(UP, 3, L)
    forwarded(DOWN, 3, L)
    turn_out(0, 2)
    for copy in pending:
        copy.wait_send()


def shards(chips, models, slope_up, slope_down, slope_norm, param_up, param_down, param_norm):
    size = slope_up.shape[-1]
    share = param_up.shape[0]
    row = jnp.concatenate(
        [slope_norm.astype(jnp.float32), jnp.pad(param_norm, (0, 128 - share))[None]], axis=1
    )
    f32, bf16 = jnp.float32, jnp.bfloat16
    any_space = pl.BlockSpec(memory_space=pl.ANY)
    vmem = pl.BlockSpec(memory_space=pltpu.VMEM)
    dma = pltpu.SemaphoreType.DMA
    half_up, half_down, next_up, next_down, half_norm, next_norm = pl.pallas_call(
        functools.partial(kernel, size, chips, models),
        name="summed_step",
        out_shape=(
            jax.ShapeDtypeStruct((size, size), bf16),
            jax.ShapeDtypeStruct((size, size), bf16),
            jax.ShapeDtypeStruct((share, size), f32),
            jax.ShapeDtypeStruct((share, size), f32),
            jax.ShapeDtypeStruct((1, size), bf16),
            jax.ShapeDtypeStruct((1, 128), f32),
        ),
        in_specs=[any_space, any_space, vmem, any_space, any_space],
        out_specs=[vmem] * 6,
        scratch_shapes=[
            pltpu.VMEM((size, size), bf16),
            pltpu.VMEM((size, size), bf16),
            pltpu.VMEM((size, size), bf16),
            pltpu.VMEM((2, chips, share, size), bf16),
            pltpu.VMEM((2, 2, 7, share, size // 2), bf16),
            pltpu.VMEM((2, 2, 7, share, size // 2), bf16),
            pltpu.VMEM((size, size), bf16),
            pltpu.VMEM((2, share, size), f32),
            pltpu.VMEM((2, share, size), f32),
            pltpu.VMEM((2, share, 128), f32),
            pltpu.VMEM((2, models - 1, share, 128), f32),
            pltpu.VMEM((2, chips, 1, size + 128), f32),
            dma((11,)),
            dma((2, 8)),
            dma((2, 8)),
            dma((2, 2, 7)),
            dma((2, 2, 7)),
            dma((2, 2, 7)),
            dma((2, 2, 7)),
            dma((2, 15)),
            dma((2, 15)),
            dma((2, models - 1)),
            dma((2, models - 1)),
            dma((2, 5)),
            dma((2, 5)),
        ],
        compiler_params=pltpu.CompilerParams(
            collective_id=0, has_side_effects=True, vmem_limit_bytes=40 * 1024 * 1024
        ),
    )(slope_up[0], slope_down[0], row, param_up, param_down.T)
    return (
        half_up,
        half_down,
        half_norm[0],
        next_up,
        next_down.T,
        next_norm[0, :share],
    )


def solution(mesh):
    chips = mesh.shape["replica"] // 2
    models = mesh.shape["model"]
    return jax.shard_map(
        functools.partial(shards, chips, models),
        mesh=mesh,
        in_specs=(
            P(("copy", "replica"), None, "model"),
            P(("copy", "replica"), "model", None),
            P(("copy", "replica"), None),
            P(("copy", "replica"), "model"),
            P(("copy", "model"), "replica"),
            P(("copy", "replica")),
        ),
        out_specs=(
            P("copy", "model"),
            P(("copy", "model"), None),
            P("copy"),
            P(("copy", "replica"), "model"),
            P(("copy", "model"), "replica"),
            P(("copy", "replica")),
        ),
        check_vma=False,
    )
```

```python
import functools

import jax
import jax.numpy as jnp
from jax import lax
from jax.experimental import pallas as pl
from jax.experimental.pallas import tpu as pltpu
from jax.sharding import PartitionSpec as P

learn_rate = 0.5
eps = 1e-06
MESH = pl.DeviceIdType.MESH
UP, DOWN = 0, 1


def kernel(
    size,
    chips,
    models,
    up_hbm,
    down_hbm,
    norm_hbm,
    param_up_hbm,
    param_down_hbm,
    gain_hbm,
    half_up,
    half_down,
    next_up,
    next_down,
    half_norm,
    next_norm,
    own_up,
    raw_down,
    own_down,
    pair_in,
    send_buf,
    recv_buf,
    gathered,
    param,
    mean,
    sizes,
    sizes_in,
    rows,
    norm_in,
    gain_in,
    load_sem,
    pair_send,
    pair_recv,
    rs_send,
    rs_recv,
    ag_send,
    ag_recv,
    fwd_send,
    fwd_recv,
    size_send,
    size_recv,
    row_send,
    row_recv,
):
    f32, bf16 = jnp.float32, jnp.bfloat16
    share = size // (2 * chips)
    cols = size // 2
    replica = lax.axis_index("replica")
    model = lax.axis_index("model")
    z, c = replica // 2, replica % 2
    partner = {"replica": z * 2 + (1 - c)}
    rate = (2 * chips) ** (-0.5)

    def chip_at(offset):
        return lax.rem(z + offset + 2 * chips, chips)

    def neighbour(d):
        return {"replica": chip_at(1 if d == 0 else -1) * 2 + c}

    def rows_of(chip, core):
        return pl.ds(pl.multiple_of((chip * 2 + core) * share, 16), share)

    def half_cols(h):
        return pl.ds(h * cols, cols)

    def rdma(src, dst, send, recv, device):
        return pltpu.make_async_remote_copy(
            src_ref=src, dst_ref=dst, send_sem=send, recv_sem=recv, device_id=device, device_id_type=MESH
        )

    own = (own_up, own_down)
    full = (half_up, gathered)
    order = (4, 3, -3, 2, -2, 1, -1, 0)

    def chip_rows(chip):
        return pl.ds(pl.multiple_of(chip * 2 * share, 32), 2 * share)

    def wait_bytes(ref, sem):
        pltpu.make_async_copy(ref, ref, sem).wait()

    def group(o):
        return 4 - abs(o)

    up_loads = {}
    for o in order:
        at = chip_rows(chip_at(o))
        sem = load_sem.at[max(group(o) - 1, 0)]
        up_loads[o] = pltpu.make_async_copy(up_hbm.at[at, :], own_up.at[at, :], sem)
    down_load = pltpu.make_async_copy(down_hbm, raw_down, load_sem.at[4])
    param_loads = [
        pltpu.make_async_copy(param_up_hbm, param.at[UP], load_sem.at[5]),
        pltpu.make_async_copy(param_down_hbm, param.at[DOWN], load_sem.at[6]),
    ]
    row_loads = [
        pltpu.make_async_copy(norm_hbm, norm_in, load_sem.at[7]),
        pltpu.make_async_copy(gain_hbm, gain_in, load_sem.at[8]),
    ]
    for o in order[:3]:
        up_loads[o].start()

    barrier = pltpu.get_barrier_semaphore()
    others = [partner, neighbour(0), neighbour(1)]
    others += [{"model": lax.rem(model + d, models)} for d in range(1, models)]
    for device in others:
        pl.semaphore_signal(barrier, inc=1, device_id=device, device_id_type=MESH)
    wait_bytes(own_up.at[0 : 6 * share, :], load_sem.at[0])
    for load in [down_load] + row_loads + [up_loads[o] for o in order[3:]] + param_loads:
        load.start()
    pl.semaphore_wait(barrier, len(others))

    def start_pairs(p, *offsets):
        for o in offsets:
            if p == UP and o in (2, 1, 0):
                wait_bytes(own_up.at[0 : (4 if o else 2) * share, :], load_sem.at[group(o) - 1])
            src = own[p].at[rows_of(chip_at(o), 1 - c), :]
            rdma(src, pair_in.at[p, o % chips], pair_send.at[0], pair_recv.at[p, group(o)], partner).start()

    ready = set()

    def pair_sum(p, o, h):
        if (p, group(o)) not in ready:
            ready.add((p, group(o)))
            wait_bytes(pair_in.at[p, 0 : 1 if o in (4, 0) else 2], pair_recv.at[p, group(o)])
        mine = own[p][rows_of(chip_at(o), c), half_cols(h)]
        return mine.astype(f32) + pair_in[p, o % chips, :, half_cols(h)].astype(f32)

    def rs_index(d, k, h):
        return 0 if k == 0 else 2 * k - 1 + (h != d)

    def rs_copy(p, d, k, h):
        i = rs_index(d, k, h)
        return rdma(send_buf.at[p, d, i], recv_buf.at[p, d, i], rs_send.at[0], rs_recv.at[p, d, i], neighbour(d))

    def rs_step(p, k, long_half):
        for d in range(2):
            h = d if long_half else 1 - d
            value = pair_sum(p, (4 - k if d == 0 else k - 4) if k else 4, h)
            if k >= 2 or (k == 1 and long_half):
                rs_copy(p, d, k - 1, h).wait_recv()
                value = value + recv_buf[p, d, rs_index(d, k - 1, h)].astype(f32)
            send_buf[p, d, rs_index(d, k, h)] = value.astype(bf16)
            rs_copy(p, d, k, h).start()

    def size_copy(p, e):
        return rdma(
            sizes.at[p],
            sizes_in.at[p, e - 1],
            size_send.at[0],
            size_recv.at[p],
            {"model": lax.rem(model + e, models)},
        )

    def finish_sum(p):
        total = jnp.zeros((share, 1), f32)
        for h in range(2):
            for d in range(2):
                rs_copy(p, d, 3, h).wait_recv()
            value = pair_sum(p, 0, h)
            for d in range(2):
                value = value + recv_buf[p, d, rs_index(d, 3, h)].astype(f32)
            value = value * rate
            mean[p, :, half_cols(h)] = value
            total = total + jnp.sum(value * value, axis=1, keepdims=True)
        param_loads[p].wait()
        weights = jnp.sum(param[p] * param[p], axis=1, keepdims=True)
        lane = lax.broadcasted_iota(jnp.int32, (share, 128), 1)
        sizes[p] = jnp.where(lane < 64, total, weights)
        for e in range(1, models):
            size_copy(p, e).start()

    def update(p):
        both = sizes[p]
        wait_bytes(sizes_in.at[p], size_recv.at[p])
        for e in range(1, models):
            both = both + sizes_in[p, e - 1]
        ratio = jnp.sqrt(both[:, 64:65]) * lax.rsqrt(both[:, 0:1] + eps)
        value = param[p] - learn_rate * (mean[p] * ratio)
        out = next_up if p == UP else next_down
        out[...] = value
        full[p][rows_of(z, c), :] = value.astype(bf16)
        at = full[p].at[rows_of(z, c), :]
        rdma(at, at, fwd_send.at[0], fwd_recv.at[forward_group(p, 0)], partner).start()

    def forward_group(p, k):
        return 0 if p == UP else k + 1

    def ag_index(d, k, h):
        return 2 * k + (h != d)

    def ag_copy(p, d, k, h, hop):
        chip = chip_at((-k - hop) if d == 0 else (k + hop))
        at = full[p].at[rows_of(chip, c), half_cols(h)]
        i = ag_index(d, k, h)
        return rdma(at, at, ag_send.at[0], ag_recv.at[p, d, i], neighbour(d))

    def forward(p, d, k, h):
        chip = chip_at((-k - 1) if d == 0 else (k + 1))
        at = full[p].at[rows_of(chip, c), half_cols(h)]
        rdma(at, at, fwd_send.at[0], fwd_recv.at[forward_group(p, k)], partner).start()

    def ag_arrive(p, k, long_half):
        for d in range(2):
            h = d if long_half else 1 - d
            ag_copy(p, d, k, h, 1).wait_recv()
            forward(p, d, k, h)

    def ag_step(p, k, long_half):
        for d in range(2):
            h = d if long_half else 1 - d
            if k:
                ag_copy(p, d, k - 1, h, 1).wait_recv()
                forward(p, d, k - 1, h)
            ag_copy(p, d, k, h, 0).start()

    def forwarded(p, k=0):
        count = chips if p == UP else (3, 2, 2, 1)[k]
        wait_bytes(pair_in.at[0, 0:count], fwd_recv.at[forward_group(p, k)])

    def row_copy(d, k, hop):
        chip = chip_at((-k - hop) if d == 0 else (k + hop))
        at = rows.at[c, chip]
        return rdma(at, at, row_send.at[0], row_recv.at[d, k], neighbour(d))

    def row_step(k):
        for d in range(2):
            if k:
                if d == 1 and k == 4:
                    continue
                row_copy(d, k - 1, 1).wait_recv()
            if k < 4 - d:
                row_copy(d, k, 0).start()

    def row_pair(core):
        return rdma(rows.at[core], rows.at[core], row_send.at[1], row_recv.at[0, 4], partner)

    def finish_rows():
        row_pair(1 - c).wait_recv()
        total = jnp.zeros((1, size), f32)
        gains = jnp.zeros((8, size), f32)
        wide = lax.broadcasted_iota(jnp.int32, (8, size), 1)
        for chip in range(chips):
            for core in range(2):
                total = total + rows[core, chip, :, :size]
                piece = jnp.broadcast_to(rows[core, chip, :, size:], (8, 128))
                piece = jnp.concatenate([piece] + [jnp.zeros((8, 128), f32)] * (size // 128 - 1), axis=1)
                start = (chip * 2 + core) * share
                moved = pltpu.roll(piece, start, 1) if start else piece
                gains = jnp.where((wide >= start) & (wide < start + share), moved, gains)
        gains = gains - learn_rate * (jnp.broadcast_to(total, (8, size)) * rate)
        half_norm[...] = gains[0].astype(bf16)
        shift = lax.rem(size - replica * share, size)
        next_norm[...] = pltpu.roll(gains, shift, 1)[0:1, 0:share]

    def turn_in(lo, hi):
        @pl.loop(lo, hi)
        def _(i):
            at = pl.ds(pl.multiple_of(i * 128, 128), 128)
            own_down[at, :] = raw_down[:, at].T

    low = (5 * chip_at(4)) // 4

    def turn_out(lo, hi):
        @pl.loop(lo, hi)
        def _(i):
            j = lax.rem(low + i, size // 128)
            at = pl.ds(pl.multiple_of(j * 128, 128), 128)
            half_down[:, at] = gathered[at, :].T

    L, S = True, False
    start_pairs(UP, 4)
    rs_step(UP, 0, L)
    start_pairs(UP, 3, -3)
    down_load.wait()
    turn_in(0, size // 128)
    rs_step(UP, 1, S)
    start_pairs(DOWN, 4, 3, -3)
    for load in row_loads:
        load.wait()
    rows[c, z, :, size:] = jnp.zeros((1, 128), jnp.float32)
    rows[c, z, :, :size] = norm_in[...].astype(jnp.float32)
    rows[c, z, :, size : size + share] = gain_in[...]
    rs_step(DOWN, 0, L)
    rs_step(DOWN, 1, S)
    start_pairs(UP, 2, -2)
    start_pairs(DOWN, 2, -2)
    rs_step(UP, 1, L)
    start_pairs(UP, 1, -1)
    start_pairs(DOWN, 1, -1)
    start_pairs(UP, 0)
    start_pairs(DOWN, 0)
    row_step(0)
    rs_step(UP, 2, S)
    rs_step(UP, 2, L)
    rs_step(DOWN, 1, L)
    rs_step(UP, 3, S)
    row_step(1)
    rs_step(UP, 3, L)
    rs_step(DOWN, 2, S)
    rs_step(DOWN, 2, L)
    row_step(2)
    finish_sum(UP)
    rs_step(DOWN, 3, S)
    update(UP)
    ag_step(UP, 0, L)
    rs_step(DOWN, 3, L)
    row_step(3)
    ag_step(UP, 0, S)
    ag_step(UP, 1, L)
    finish_sum(DOWN)
    ag_step(UP, 1, S)
    row_step(4)
    row_pair(c).start()
    update(DOWN)
    ag_step(DOWN, 0, L)
    ag_step(DOWN, 0, S)
    ag_step(UP, 2, L)
    ag_step(DOWN, 1, L)
    ag_step(DOWN, 1, S)
    finish_rows()
    ag_step(UP, 2, S)
    ag_step(DOWN, 2, L)
    ag_step(DOWN, 2, S)
    forwarded(DOWN, 0)
    turn_out(5, 7)
    ag_step(DOWN, 3, L)
    ag_step(UP, 3, L)
    forwarded(DOWN, 1)
    turn_out(4, 5)
    turn_out(7, 8)
    ag_arrive(UP, 2, S)
    ag_arrive(DOWN, 2, S)
    forwarded(DOWN, 2)
    turn_out(2, 4)
    turn_out(8, 10)
    ag_arrive(DOWN, 3, L)
    forwarded(DOWN, 3)
    turn_out(0, 2)
    ag_arrive(UP, 3, L)
    forwarded(UP)
    wait_bytes(pair_in, pair_send.at[0])
    wait_bytes(send_buf, rs_send.at[0])
    wait_bytes(send_buf, ag_send.at[0])
    wait_bytes(pair_in, fwd_send.at[0])
    wait_bytes(sizes_in, size_send.at[0])
    wait_bytes(rows.at[0, 0 : chips - 1], row_send.at[0])
    wait_bytes(rows.at[0], row_send.at[1])


def put(*refs):
    count = len(refs) // 2
    copies = [pltpu.make_async_copy(refs[i], refs[count + i], refs[-1].at[i]) for i in range(count)]
    for copy in copies:
        copy.start()
    for copy in copies:
        copy.wait()


def shards(chips, models, slope_up, slope_down, slope_norm, param_up, param_down, param_norm):
    size = slope_up.shape[-1]
    share = param_up.shape[0]
    f32, bf16 = jnp.float32, jnp.bfloat16
    hbm = pl.BlockSpec(memory_space=pltpu.HBM)
    vmem = pl.BlockSpec(memory_space=pltpu.VMEM)
    dma = pltpu.SemaphoreType.DMA
    results = (
        jax.ShapeDtypeStruct((size, size), bf16),
        jax.ShapeDtypeStruct((size, size), bf16),
        jax.ShapeDtypeStruct((share, size), f32),
        jax.ShapeDtypeStruct((share, size), f32),
        jax.ShapeDtypeStruct((size,), bf16),
        jax.ShapeDtypeStruct((1, share), f32),
    )
    arrays = (slope_up[0], slope_down[0], slope_norm, param_up, param_down.T, param_norm[None])
    made = pl.pallas_call(
        functools.partial(kernel, size, chips, models),
        name="summed_step",
        out_shape=tuple(pltpu.VMEM(r.shape, r.dtype) for r in results),
        in_specs=[hbm] * 6,
        out_specs=[vmem] * 6,
        scratch_shapes=[
            pltpu.VMEM((size, size), bf16),
            pltpu.VMEM((size, size), bf16),
            pltpu.VMEM((size, size), bf16),
            pltpu.VMEM((2, chips, share, size), bf16),
            pltpu.VMEM((2, 2, 7, share, size // 2), bf16),
            pltpu.VMEM((2, 2, 7, share, size // 2), bf16),
            pltpu.VMEM((size, size), bf16),
            pltpu.VMEM((2, share, size), f32),
            pltpu.VMEM((2, share, size), f32),
            pltpu.VMEM((2, share, 128), f32),
            pltpu.VMEM((2, models - 1, share, 128), f32),
            pltpu.VMEM((2, chips, 1, size + 128), f32),
            pltpu.VMEM((1, size), bf16),
            pltpu.VMEM((1, share), f32),
            dma((9,)),
            dma((1,)),
            dma((2, 5)),
            dma((1,)),
            dma((2, 2, 7)),
            dma((1,)),
            dma((2, 2, 7)),
            dma((1,)),
            dma((5,)),
            dma((1,)),
            dma((2,)),
            dma((2,)),
            dma((2, 5)),
        ],
        compiler_params=pltpu.CompilerParams(
            collective_id=0, has_side_effects=True, vmem_limit_bytes=48 * 1024 * 1024
        ),
    )(*(pltpu.with_memory_space_constraint(a, pltpu.HBM) for a in arrays))
    half_up, half_down, next_up, next_down, half_norm, next_norm = pl.pallas_call(
        put,
        name="put",
        out_shape=results,
        in_specs=[vmem] * 6,
        out_specs=[hbm] * 6,
        scratch_shapes=[dma((6,))],
        compiler_params=pltpu.CompilerParams(vmem_limit_bytes=1024 * 1024),
    )(*made)
    return (half_up, half_down, half_norm, next_up, next_down.T, next_norm[0])


def solution(mesh):
    chips = mesh.shape["replica"] // 2
    models = mesh.shape["model"]
    return jax.shard_map(
        functools.partial(shards, chips, models),
        mesh=mesh,
        in_specs=(
            P(("copy", "replica"), None, "model"),
            P(("copy", "replica"), "model", None),
            P(("copy", "replica"), None),
            P(("copy", "replica"), "model"),
            P(("copy", "model"), "replica"),
            P(("copy", "replica")),
        ),
        out_specs=(
            P("copy", "model"),
            P(("copy", "model"), None),
            P("copy"),
            P(("copy", "replica"), "model"),
            P(("copy", "model"), "replica"),
            P(("copy", "replica")),
        ),
        check_vma=False,
    )
```

```python
import functools

import jax
import jax.numpy as jnp
from jax import lax
from jax.experimental import pallas as pl
from jax.experimental.pallas import tpu as pltpu
from jax.sharding import PartitionSpec as P

learn_rate = 0.5
eps = 1e-06
MESH = pl.DeviceIdType.MESH
UP, DOWN = 0, 1


def kernel(
    size,
    chips,
    models,
    up_hbm,
    down_hbm,
    norm_hbm,
    param_up_hbm,
    param_down_hbm,
    gain_hbm,
    half_up,
    half_down,
    next_up,
    next_down,
    half_norm,
    next_norm,
    own_up,
    raw_down,
    own_down,
    pair_in,
    send_buf,
    recv_buf,
    gathered,
    param,
    mean,
    sizes,
    sizes_in,
    rows,
    norm_in,
    gain_in,
    load_sem,
    pair_send,
    pair_recv,
    rs_send,
    rs_recv,
    ag_send,
    ag_recv,
    fwd_send,
    fwd_recv,
    size_send,
    size_recv,
    row_send,
    row_recv,
    last_sem,
):
    f32, bf16 = jnp.float32, jnp.bfloat16
    share = size // (2 * chips)
    cols = size // 2
    replica = lax.axis_index("replica")
    model = lax.axis_index("model")
    z, c = replica // 2, replica % 2
    partner = {"replica": z * 2 + (1 - c)}
    rate = (2 * chips) ** (-0.5)

    def chip_at(offset):
        return lax.rem(z + offset + 2 * chips, chips)

    def neighbour(d):
        return {"replica": chip_at(1 if d == 0 else -1) * 2 + c}

    def rows_of(chip, core):
        return pl.ds(pl.multiple_of((chip * 2 + core) * share, 16), share)

    def half_cols(h):
        return pl.ds(h * cols, cols)

    def rdma(src, dst, send, recv, device):
        return pltpu.make_async_remote_copy(
            src_ref=src, dst_ref=dst, send_sem=send, recv_sem=recv, device_id=device, device_id_type=MESH
        )

    own = (own_up, own_down)
    full = (half_up, gathered)
    order = (4, 3, -3, 2, -2, 1, -1, 0)

    def chip_rows(chip):
        return pl.ds(pl.multiple_of(chip * 2 * share, 32), 2 * share)

    def wait_bytes(ref, sem):
        pltpu.make_async_copy(ref, ref, sem).wait()

    def group(o):
        return 4 - abs(o)

    up_loads = {}
    for o in order:
        at = chip_rows(chip_at(o))
        sem = load_sem.at[group(o)]
        up_loads[o] = pltpu.make_async_copy(up_hbm.at[at, :], own_up.at[at, :], sem)
    down_load = pltpu.make_async_copy(down_hbm, raw_down, load_sem.at[5])
    param_loads = [
        pltpu.make_async_copy(param_up_hbm, param.at[UP], load_sem.at[6]),
        pltpu.make_async_copy(param_down_hbm, param.at[DOWN], load_sem.at[7]),
    ]
    row_loads = [
        pltpu.make_async_copy(norm_hbm, norm_in, load_sem.at[8]),
        pltpu.make_async_copy(gain_hbm, gain_in, load_sem.at[9]),
    ]
    up_loads[4].start()

    barrier = pltpu.get_barrier_semaphore()
    others = [partner, neighbour(0), neighbour(1)]
    others += [{"model": lax.rem(model + d, models)} for d in range(1, models)]
    for device in others:
        pl.semaphore_signal(barrier, inc=1, device_id=device, device_id_type=MESH)
    up_loads[3].start()
    up_loads[-3].start()
    up_loads[4].wait()
    for load in [down_load] + row_loads + [up_loads[o] for o in order[3:]] + param_loads:
        load.start()
    pl.semaphore_wait(barrier, len(others))

    def start_pairs(p, *offsets):
        for o in offsets:
            if p == UP and o in (3, 2, 1, 0):
                wait_bytes(own_up.at[0 : (4 if o else 2) * share, :], load_sem.at[group(o)])
            src = own[p].at[rows_of(chip_at(o), 1 - c), :]
            rdma(src, pair_in.at[p, o % chips], pair_send.at[0], pair_recv.at[p, group(o)], partner).start()

    ready = set()

    def pair_sum(p, o, h):
        if (p, group(o)) not in ready:
            ready.add((p, group(o)))
            wait_bytes(pair_in.at[p, 0 : 1 if o in (4, 0) else 2], pair_recv.at[p, group(o)])
        mine = own[p][rows_of(chip_at(o), c), half_cols(h)]
        return mine.astype(f32) + pair_in[p, o % chips, :, half_cols(h)].astype(f32)

    def rs_index(d, k, h):
        return 0 if k == 0 else 2 * k - 1 + (h != d)

    def rs_copy(p, d, k, h):
        i = rs_index(d, k, h)
        return rdma(send_buf.at[p, d, i], recv_buf.at[p, d, i], rs_send.at[0], rs_recv.at[p, d, i], neighbour(d))

    def rs_step(p, k, long_half):
        for d in range(2):
            h = d if long_half else 1 - d
            value = pair_sum(p, (4 - k if d == 0 else k - 4) if k else 4, h)
            if k >= 2 or (k == 1 and long_half):
                rs_copy(p, d, k - 1, h).wait_recv()
                value = value + recv_buf[p, d, rs_index(d, k - 1, h)].astype(f32)
            send_buf[p, d, rs_index(d, k, h)] = value.astype(bf16)
            rs_copy(p, d, k, h).start()

    def size_copy(p, e):
        return rdma(
            sizes.at[p],
            sizes_in.at[p, e - 1],
            size_send.at[0],
            size_recv.at[p],
            {"model": lax.rem(model + e, models)},
        )

    def finish_sum(p):
        total = jnp.zeros((share, 1), f32)
        for h in range(2):
            for d in range(2):
                rs_copy(p, d, 3, h).wait_recv()
            value = pair_sum(p, 0, h)
            for d in range(2):
                value = value + recv_buf[p, d, rs_index(d, 3, h)].astype(f32)
            value = value * rate
            mean[p, :, half_cols(h)] = value
            total = total + jnp.sum(value * value, axis=1, keepdims=True)
        param_loads[p].wait()
        weights = jnp.sum(param[p] * param[p], axis=1, keepdims=True)
        lane = lax.broadcasted_iota(jnp.int32, (share, 128), 1)
        sizes[p] = jnp.where(lane < 64, total, weights)
        for e in range(1, models):
            size_copy(p, e).start()

    def update(p):
        both = sizes[p]
        wait_bytes(sizes_in.at[p], size_recv.at[p])
        for e in range(1, models):
            both = both + sizes_in[p, e - 1]
        ratio = jnp.sqrt(both[:, 64:65]) * lax.rsqrt(both[:, 0:1] + eps)
        value = param[p] - learn_rate * (mean[p] * ratio)
        out = next_up if p == UP else next_down
        out[...] = value
        full[p][rows_of(z, c), :] = value.astype(bf16)
        at = full[p].at[rows_of(z, c), :]
        rdma(at, at, fwd_send.at[0], fwd_recv.at[forward_group(p, 0)], partner).start()

    def forward_group(p, k, long_half=False):
        return (5 if k == 2 and long_half else 0) if p == UP else k + 1

    def ag_index(d, k, h):
        return 2 * k + (h != d)

    def ag_copy(p, d, k, h, hop):
        chip = chip_at((-k - hop) if d == 0 else (k + hop))
        at = full[p].at[rows_of(chip, c), half_cols(h)]
        i = ag_index(d, k, h)
        return rdma(at, at, ag_send.at[0], ag_recv.at[p, i], neighbour(d))

    def forward(p, d, k, h):
        chip = chip_at((-k - 1) if d == 0 else (k + 1))
        at = full[p].at[rows_of(chip, c), half_cols(h)]
        rdma(at, at, fwd_send.at[0], fwd_recv.at[forward_group(p, k, h == d)], partner).start()

    def ag_wait(p, k, long_half):
        wait_bytes(send_buf.at[0, 0, 0:2], ag_recv.at[p, 2 * k + (not long_half)])
        for d in range(2):
            forward(p, d, k, d if long_half else 1 - d)

    def ag_step(p, k, long_half):
        if k:
            ag_wait(p, k - 1, long_half)
        for d in range(2):
            ag_copy(p, d, k, d if long_half else 1 - d, 0).start()

    def forwarded(p, k=0):
        count = chips - 2 if p == UP else (3, 2, 2, 1)[k]
        wait_bytes(pair_in.at[0, 0:count], fwd_recv.at[forward_group(p, k)])

    def last_rows(d, hop):
        chip = chip_at((-3 - hop) if d == 0 else (3 + hop))
        return full[UP].at[chip_rows(chip), half_cols(d)]

    def last_send():
        @pl.when(c == 1)
        def _():
            wait_bytes(pair_in.at[0, 0:1], fwd_recv.at[5])
            for d in range(2):
                at = last_rows(d, 0)
                rdma(at, at, last_sem.at[0], last_sem.at[1], neighbour(d)).start()

    def last_wait():
        @pl.when(c == 1)
        def _():
            wait_bytes(pair_in.at[0, 0:2], last_sem.at[1])
            for d in range(2):
                at = last_rows(d, 1)
                rdma(at, at, last_sem.at[2], last_sem.at[3], partner).start()

    def last_done():
        @pl.when(c == 1)
        def _():
            wait_bytes(pair_in.at[0, 0:2], last_sem.at[0])
            wait_bytes(pair_in.at[0, 0:2], last_sem.at[2])

        @pl.when(c == 0)
        def _():
            wait_bytes(pair_in.at[0, 0:1], fwd_recv.at[5])
            wait_bytes(pair_in.at[0, 0:2], last_sem.at[3])

    def row_copy(d, k, hop):
        chip = chip_at((-k - hop) if d == 0 else (k + hop))
        at = rows.at[c, chip]
        return rdma(at, at, row_send.at[0], row_recv.at[d * 4 + k], neighbour(d))

    def row_step(k):
        for d in range(2):
            if k:
                if d == 1 and k == 4:
                    continue
                row_copy(d, k - 1, 1).wait_recv()
            if k < 4 - d:
                row_copy(d, k, 0).start()

    def row_pair(core):
        return rdma(rows.at[core], rows.at[core], row_send.at[1], row_recv.at[7], partner)

    def finish_rows():
        row_pair(1 - c).wait_recv()
        total = jnp.zeros((1, size), f32)
        gains = jnp.zeros((8, size), f32)
        wide = lax.broadcasted_iota(jnp.int32, (8, size), 1)
        for chip in range(chips):
            for core in range(2):
                total = total + rows[core, chip, :, :size]
                piece = jnp.broadcast_to(rows[core, chip, :, size:], (8, 128))
                piece = jnp.concatenate([piece] + [jnp.zeros((8, 128), f32)] * (size // 128 - 1), axis=1)
                start = (chip * 2 + core) * share
                moved = pltpu.roll(piece, start, 1) if start else piece
                gains = jnp.where((wide >= start) & (wide < start + share), moved, gains)
        gains = gains - learn_rate * (jnp.broadcast_to(total, (8, size)) * rate)
        half_norm[...] = gains[0].astype(bf16)
        shift = lax.rem(size - replica * share, size)
        next_norm[...] = pltpu.roll(gains, shift, 1)[0:1, 0:share]

    def turn_in(lo, hi):
        @pl.loop(lo, hi)
        def _(i):
            at = pl.ds(pl.multiple_of(i * 128, 128), 128)
            own_down[at, :] = raw_down[:, at].T

    low = (5 * chip_at(4)) // 4

    def turn_out(lo, hi):
        @pl.loop(lo, hi)
        def _(i):
            j = lax.rem(low + i, size // 128)
            at = pl.ds(pl.multiple_of(j * 128, 128), 128)
            half_down[:, at] = gathered[at, :].T

    L, S = True, False
    start_pairs(UP, 4)
    rs_step(UP, 0, L)
    start_pairs(UP, 3, -3)
    down_load.wait()
    turn_in(0, size // 128)
    rs_step(UP, 1, S)
    start_pairs(DOWN, 4, 3, -3)
    for load in row_loads:
        load.wait()
    rows[c, z, :, size:] = jnp.zeros((1, 128), jnp.float32)
    rows[c, z, :, :size] = norm_in[...].astype(jnp.float32)
    rows[c, z, :, size : size + share] = gain_in[...]
    rs_step(DOWN, 0, L)
    rs_step(DOWN, 1, S)
    start_pairs(UP, 2, -2)
    start_pairs(DOWN, 2, -2)
    rs_step(UP, 1, L)
    start_pairs(UP, 1, -1)
    start_pairs(DOWN, 1, -1)
    start_pairs(UP, 0)
    start_pairs(DOWN, 0)
    row_step(0)
    rs_step(UP, 2, S)
    rs_step(UP, 2, L)
    rs_step(DOWN, 1, L)
    rs_step(UP, 3, S)
    row_step(1)
    rs_step(UP, 3, L)
    rs_step(DOWN, 2, S)
    rs_step(DOWN, 2, L)
    row_step(2)
    finish_sum(UP)
    rs_step(DOWN, 3, S)
    update(UP)
    ag_step(UP, 0, L)
    rs_step(DOWN, 3, L)
    row_step(3)
    ag_step(UP, 0, S)
    ag_step(UP, 1, L)
    finish_sum(DOWN)
    ag_step(UP, 1, S)
    row_step(4)
    row_pair(c).start()
    update(DOWN)
    ag_step(DOWN, 0, L)
    ag_step(DOWN, 0, S)
    ag_step(UP, 2, L)
    ag_step(DOWN, 1, L)
    ag_step(DOWN, 1, S)
    finish_rows()
    ag_step(UP, 2, S)
    ag_wait(UP, 2, L)
    ag_step(DOWN, 2, L)
    ag_step(DOWN, 2, S)
    forwarded(DOWN, 0)
    turn_out(5, 7)
    ag_step(DOWN, 3, L)
    last_send()
    ag_wait(UP, 2, S)
    forwarded(DOWN, 1)
    turn_out(4, 5)
    turn_out(7, 8)
    ag_wait(DOWN, 2, S)
    forwarded(DOWN, 2)
    turn_out(2, 4)
    turn_out(8, 10)
    ag_wait(DOWN, 3, L)
    last_wait()
    forwarded(DOWN, 3)
    turn_out(0, 2)
    forwarded(UP)
    last_done()
    wait_bytes(pair_in, pair_send.at[0])
    wait_bytes(send_buf, rs_send.at[0])
    wait_bytes(own_up.at[0 : 13 * share, :], ag_send.at[0])
    wait_bytes(own_up.at[0 : 15 * share, :], fwd_send.at[0])
    wait_bytes(sizes_in, size_send.at[0])
    wait_bytes(rows.at[0, 0 : chips - 1], row_send.at[0])
    wait_bytes(rows.at[0], row_send.at[1])


def put(*refs):
    count = len(refs) // 2
    copies = [pltpu.make_async_copy(refs[i], refs[count + i], refs[-1].at[i]) for i in range(count)]
    for copy in copies:
        copy.start()
    for copy in copies:
        copy.wait()


def shards(chips, models, slope_up, slope_down, slope_norm, param_up, param_down, param_norm):
    size = slope_up.shape[-1]
    share = param_up.shape[0]
    f32, bf16 = jnp.float32, jnp.bfloat16
    hbm = pl.BlockSpec(memory_space=pltpu.HBM)
    vmem = pl.BlockSpec(memory_space=pltpu.VMEM)
    dma = pltpu.SemaphoreType.DMA
    results = (
        jax.ShapeDtypeStruct((size, size), bf16),
        jax.ShapeDtypeStruct((size, size), bf16),
        jax.ShapeDtypeStruct((share, size), f32),
        jax.ShapeDtypeStruct((share, size), f32),
        jax.ShapeDtypeStruct((size,), bf16),
        jax.ShapeDtypeStruct((1, share), f32),
    )
    arrays = (slope_up[0], slope_down[0], slope_norm, param_up, param_down.T, param_norm[None])
    made = pl.pallas_call(
        functools.partial(kernel, size, chips, models),
        name="summed_step",
        out_shape=tuple(pltpu.VMEM(r.shape, r.dtype) for r in results),
        in_specs=[hbm] * 6,
        out_specs=[vmem] * 6,
        scratch_shapes=[
            pltpu.VMEM((size, size), bf16),
            pltpu.VMEM((size, size), bf16),
            pltpu.VMEM((size, size), bf16),
            pltpu.VMEM((2, chips, share, size), bf16),
            pltpu.VMEM((2, 2, 7, share, size // 2), bf16),
            pltpu.VMEM((2, 2, 7, share, size // 2), bf16),
            pltpu.VMEM((size, size), bf16),
            pltpu.VMEM((2, share, size), f32),
            pltpu.VMEM((2, share, size), f32),
            pltpu.VMEM((2, share, 128), f32),
            pltpu.VMEM((2, models - 1, share, 128), f32),
            pltpu.VMEM((2, chips, 1, size + 128), f32),
            pltpu.VMEM((1, size), bf16),
            pltpu.VMEM((1, share), f32),
            dma((10,)),
            dma((1,)),
            dma((2, 5)),
            dma((1,)),
            dma((2, 2, 7)),
            dma((1,)),
            dma((2, 7)),
            dma((1,)),
            dma((6,)),
            dma((1,)),
            dma((2,)),
            dma((2,)),
            dma((8,)),
            dma((4,)),
        ],
        compiler_params=pltpu.CompilerParams(
            collective_id=0, has_side_effects=True, vmem_limit_bytes=48 * 1024 * 1024
        ),
    )(*(pltpu.with_memory_space_constraint(a, pltpu.HBM) for a in arrays))
    half_up, half_down, next_up, next_down, half_norm, next_norm = pl.pallas_call(
        put,
        name="put",
        out_shape=results,
        in_specs=[vmem] * 6,
        out_specs=[hbm] * 6,
        scratch_shapes=[dma((6,))],
        compiler_params=pltpu.CompilerParams(vmem_limit_bytes=1024 * 1024),
    )(*made)
    return (half_up, half_down, half_norm, next_up, next_down.T, next_norm[0])


def solution(mesh):
    chips = mesh.shape["replica"] // 2
    models = mesh.shape["model"]
    return jax.shard_map(
        functools.partial(shards, chips, models),
        mesh=mesh,
        in_specs=(
            P(("copy", "replica"), None, "model"),
            P(("copy", "replica"), "model", None),
            P(("copy", "replica"), None),
            P(("copy", "replica"), "model"),
            P(("copy", "model"), "replica"),
            P(("copy", "replica")),
        ),
        out_specs=(
            P("copy", "model"),
            P(("copy", "model"), None),
            P("copy"),
            P(("copy", "replica"), "model"),
            P(("copy", "model"), "replica"),
            P(("copy", "replica")),
        ),
        check_vma=False,
    )
```

```python
import functools

import jax
import jax.numpy as jnp
from jax import lax
from jax.experimental import pallas as pl
from jax.experimental.pallas import tpu as pltpu
from jax.sharding import PartitionSpec as P

learn_rate = 0.5
eps = 1e-06
MESH = pl.DeviceIdType.MESH
UP, DOWN = 0, 1


def kernel(
    size,
    chips,
    models,
    up_hbm,
    down_hbm,
    norm_hbm,
    param_up_hbm,
    param_down_hbm,
    gain_hbm,
    half_up,
    half_down,
    next_up,
    next_down,
    half_norm,
    next_norm,
    own_up,
    raw_down,
    own_down,
    pair_in,
    send_buf,
    recv_buf,
    gathered,
    param,
    mean,
    sizes,
    sizes_in,
    rows,
    norm_in,
    gain_in,
    load_sem,
    pair_send,
    pair_recv,
    rs_send,
    rs_recv,
    ag_send,
    ag_recv,
    fwd_send,
    fwd_recv,
    size_send,
    size_recv,
    row_send,
    row_recv,
    last_sem,
):
    f32, bf16 = jnp.float32, jnp.bfloat16
    share = size // (2 * chips)
    cols = size // 2
    replica = lax.axis_index("replica")
    model = lax.axis_index("model")
    z, c = replica // 2, replica % 2
    partner = {"replica": z * 2 + (1 - c)}
    rate = (2 * chips) ** (-0.5)

    def chip_at(offset):
        return lax.rem(z + offset + 2 * chips, chips)

    def neighbour(d):
        return {"replica": chip_at(1 if d == 0 else -1) * 2 + c}

    def rows_of(chip, core):
        return pl.ds(pl.multiple_of((chip * 2 + core) * share, 16), share)

    def half_cols(h):
        return pl.ds(h * cols, cols)

    def rdma(src, dst, send, recv, device):
        return pltpu.make_async_remote_copy(
            src_ref=src, dst_ref=dst, send_sem=send, recv_sem=recv, device_id=device, device_id_type=MESH
        )

    own = (own_up, own_down)
    full = (half_up, gathered)
    order = (4, 3, -3, 2, -2, 1, -1, 0)

    def chip_rows(chip):
        return pl.ds(pl.multiple_of(chip * 2 * share, 32), 2 * share)

    def wait_bytes(ref, sem):
        pltpu.make_async_copy(ref, ref, sem).wait()

    def group(o):
        return 4 - abs(o)

    up_loads = {}
    for o in order:
        at = chip_rows(chip_at(o))
        sem = load_sem.at[group(o)]
        up_loads[o] = pltpu.make_async_copy(up_hbm.at[at, :], own_up.at[at, :], sem)
    down_load = pltpu.make_async_copy(down_hbm, raw_down, load_sem.at[5])
    param_loads = [
        pltpu.make_async_copy(param_up_hbm, param.at[UP], load_sem.at[6]),
        pltpu.make_async_copy(param_down_hbm, param.at[DOWN], load_sem.at[7]),
    ]
    row_loads = [
        pltpu.make_async_copy(norm_hbm, norm_in, load_sem.at[8]),
        pltpu.make_async_copy(gain_hbm, gain_in, load_sem.at[9]),
    ]
    for load in [up_loads[4]] + row_loads:
        load.start()

    barrier = pltpu.get_barrier_semaphore()
    others = [partner, neighbour(0), neighbour(1)]
    others += [{"model": lax.rem(model + d, models)} for d in range(1, models)]
    for device in others:
        pl.semaphore_signal(barrier, inc=1, device_id=device, device_id_type=MESH)
    up_loads[3].start()
    up_loads[-3].start()
    up_loads[4].wait()
    for load in [down_load] + [up_loads[o] for o in order[3:]] + param_loads:
        load.start()
    pl.semaphore_wait(barrier, len(others))

    def start_pairs(p, *offsets):
        for o in offsets:
            if p == UP and o in (3, 2, 1, 0):
                wait_bytes(own_up.at[0 : (4 if o else 2) * share, :], load_sem.at[group(o)])
            src = own[p].at[rows_of(chip_at(o), 1 - c), :]
            rdma(src, pair_in.at[p, o % chips], pair_send.at[0], pair_recv.at[p, group(o)], partner).start()

    ready = set()

    def pair_sum(p, o, h):
        if (p, group(o)) not in ready:
            ready.add((p, group(o)))
            wait_bytes(pair_in.at[p, 0 : 1 if o in (4, 0) else 2], pair_recv.at[p, group(o)])
        mine = own[p][rows_of(chip_at(o), c), half_cols(h)]
        return mine.astype(f32) + pair_in[p, o % chips, :, half_cols(h)].astype(f32)

    def rs_index(d, k, h):
        return 0 if k == 0 else 2 * k - 1 + (h != d)

    def rs_copy(p, d, k, h):
        i = rs_index(d, k, h)
        return rdma(send_buf.at[p, d, i], recv_buf.at[p, d, i], rs_send.at[0], rs_recv.at[p, d, i], neighbour(d))

    def rs_step(p, k, long_half):
        for d in range(2):
            h = d if long_half else 1 - d
            value = pair_sum(p, (4 - k if d == 0 else k - 4) if k else 4, h)
            if k >= 2 or (k == 1 and long_half):
                rs_copy(p, d, k - 1, h).wait_recv()
                value = value + recv_buf[p, d, rs_index(d, k - 1, h)].astype(f32)
            send_buf[p, d, rs_index(d, k, h)] = value.astype(bf16)
            rs_copy(p, d, k, h).start()

    def size_copy(p, e):
        return rdma(
            sizes.at[p],
            sizes_in.at[p, e - 1],
            size_send.at[0],
            size_recv.at[p],
            {"model": lax.rem(model + e, models)},
        )

    def finish_sum(p):
        total = jnp.zeros((share, 1), f32)
        for h in range(2):
            for d in range(2):
                rs_copy(p, d, 3, h).wait_recv()
            value = pair_sum(p, 0, h)
            for d in range(2):
                value = value + recv_buf[p, d, rs_index(d, 3, h)].astype(f32)
            value = value * rate
            mean[p, :, half_cols(h)] = value
            total = total + jnp.sum(value * value, axis=1, keepdims=True)
        param_loads[p].wait()
        weights = jnp.sum(param[p] * param[p], axis=1, keepdims=True)
        lane = lax.broadcasted_iota(jnp.int32, (share, 128), 1)
        sizes[p] = jnp.where(lane < 64, total, weights)
        for e in range(1, models):
            size_copy(p, e).start()

    def update(p):
        both = sizes[p]
        wait_bytes(sizes_in.at[p], size_recv.at[p])
        for e in range(1, models):
            both = both + sizes_in[p, e - 1]
        ratio = jnp.sqrt(both[:, 64:65]) * lax.rsqrt(both[:, 0:1] + eps)
        value = param[p] - learn_rate * (mean[p] * ratio)
        out = next_up if p == UP else next_down
        out[...] = value
        full[p][rows_of(z, c), :] = value.astype(bf16)
        at = full[p].at[rows_of(z, c), :]
        rdma(at, at, fwd_send.at[0], fwd_recv.at[forward_group(p, 0)], partner).start()

    def forward_group(p, k, long_half=False):
        return (5 if k == 2 and long_half else 0) if p == UP else k + 1

    def ag_index(d, k, h):
        return 2 * k + (h != d)

    def ag_copy(p, d, k, h, hop):
        chip = chip_at((-k - hop) if d == 0 else (k + hop))
        at = full[p].at[rows_of(chip, c), half_cols(h)]
        i = ag_index(d, k, h)
        return rdma(at, at, ag_send.at[0], ag_recv.at[p, d, i], neighbour(d))

    def forward(p, d, k, h):
        chip = chip_at((-k - 1) if d == 0 else (k + 1))
        at = full[p].at[rows_of(chip, c), half_cols(h)]
        rdma(at, at, fwd_send.at[0], fwd_recv.at[forward_group(p, k, h == d)], partner).start()

    def ag_wait(p, k, long_half, onward=False):
        for d in range(2):
            h = d if long_half else 1 - d
            ag_copy(p, d, k, h, 1).wait_recv()
            forward(p, d, k, h)
            if onward:
                ag_copy(p, d, k + 1, h, 0).start()

    def ag_step(p, k, long_half):
        if k:
            ag_wait(p, k - 1, long_half, True)
        else:
            for d in range(2):
                ag_copy(p, d, k, d if long_half else 1 - d, 0).start()

    def forwarded(p, k=0):
        count = chips - 2 if p == UP else (3, 2, 2, 1)[k]
        wait_bytes(pair_in.at[0, 0:count], fwd_recv.at[forward_group(p, k)])

    def last_rows(d, hop):
        chip = chip_at((-3 - hop) if d == 0 else (3 + hop))
        return full[UP].at[chip_rows(chip), half_cols(d)]

    def last_send():
        @pl.when(c == 1)
        def _():
            wait_bytes(pair_in.at[0, 0:1], fwd_recv.at[5])
            for d in range(2):
                at = last_rows(d, 0)
                rdma(at, at, last_sem.at[0], last_sem.at[1], neighbour(d)).start()

    def last_wait():
        @pl.when(c == 1)
        def _():
            wait_bytes(pair_in.at[0, 0:2], last_sem.at[1])
            for d in range(2):
                at = last_rows(d, 1)
                rdma(at, at, last_sem.at[2], last_sem.at[3], partner).start()

    def last_done():
        @pl.when(c == 1)
        def _():
            wait_bytes(pair_in.at[0, 0:2], last_sem.at[0])
            wait_bytes(pair_in.at[0, 0:2], last_sem.at[2])

        @pl.when(c == 0)
        def _():
            wait_bytes(pair_in.at[0, 0:1], fwd_recv.at[5])
            wait_bytes(pair_in.at[0, 0:2], last_sem.at[3])

    def row_copy(d, k, hop):
        chip = chip_at((-k - hop) if d == 0 else (k + hop))
        at = rows.at[c, chip]
        return rdma(at, at, row_send.at[0], row_recv.at[d * 4 + k], neighbour(d))

    def row_step(k):
        for d in range(2):
            if k:
                if d == 1 and k == 4:
                    continue
                row_copy(d, k - 1, 1).wait_recv()
            if k < 4 - d:
                row_copy(d, k, 0).start()

    def row_pair(core):
        return rdma(rows.at[core], rows.at[core], row_send.at[1], row_recv.at[7], partner)

    def finish_rows():
        row_pair(1 - c).wait_recv()
        total = jnp.zeros((1, size), f32)
        gains = jnp.zeros((8, size), f32)
        wide = lax.broadcasted_iota(jnp.int32, (8, size), 1)
        for chip in range(chips):
            for core in range(2):
                total = total + rows[core, chip, :, :size]
                piece = jnp.broadcast_to(rows[core, chip, :, size:], (8, 128))
                piece = jnp.concatenate([piece] + [jnp.zeros((8, 128), f32)] * (size // 128 - 1), axis=1)
                start = (chip * 2 + core) * share
                moved = pltpu.roll(piece, start, 1) if start else piece
                gains = jnp.where((wide >= start) & (wide < start + share), moved, gains)
        gains = gains - learn_rate * (jnp.broadcast_to(total, (8, size)) * rate)
        half_norm[...] = gains[0].astype(bf16)
        shift = lax.rem(size - replica * share, size)
        next_norm[...] = pltpu.roll(gains, shift, 1)[0:1, 0:share]

    def turn_in(lo, hi):
        @pl.loop(lo, hi)
        def _(i):
            at = pl.ds(pl.multiple_of(i * 128, 128), 128)
            own_down[at, :] = raw_down[:, at].T

    low = (5 * chip_at(4)) // 4

    def turn_out(lo, hi):
        @pl.loop(lo, hi)
        def _(i):
            j = lax.rem(low + i, size // 128)
            at = pl.ds(pl.multiple_of(j * 128, 128), 128)
            half_down[:, at] = gathered[at, :].T

    L, S = True, False
    start_pairs(UP, 4)
    for load in row_loads:
        load.wait()
    rows[c, z, :, size:] = jnp.zeros((1, 128), jnp.float32)
    rows[c, z, :, :size] = norm_in[...].astype(jnp.float32)
    rows[c, z, :, size : size + share] = gain_in[...]
    row_step(0)
    rs_step(UP, 0, L)
    start_pairs(UP, 3, -3)
    down_load.wait()
    turn_in(0, size // 128)
    rs_step(UP, 1, S)
    start_pairs(DOWN, 4, 3, -3)
    rs_step(DOWN, 0, L)
    rs_step(DOWN, 1, S)
    start_pairs(UP, 2, -2)
    start_pairs(DOWN, 2, -2)
    rs_step(UP, 1, L)
    start_pairs(UP, 1, -1)
    start_pairs(DOWN, 1, -1)
    start_pairs(UP, 0)
    start_pairs(DOWN, 0)
    rs_step(UP, 2, S)
    rs_step(UP, 2, L)
    rs_step(DOWN, 1, L)
    rs_step(UP, 3, S)
    row_step(1)
    rs_step(UP, 3, L)
    rs_step(DOWN, 2, S)
    rs_step(DOWN, 2, L)
    row_step(2)
    finish_sum(UP)
    rs_step(DOWN, 3, S)
    update(UP)
    ag_step(UP, 0, L)
    rs_step(DOWN, 3, L)
    row_step(3)
    ag_step(UP, 0, S)
    ag_step(UP, 1, L)
    finish_sum(DOWN)
    ag_step(UP, 1, S)
    row_step(4)
    row_pair(c).start()
    update(DOWN)
    ag_step(DOWN, 0, L)
    ag_step(DOWN, 0, S)
    ag_step(UP, 2, L)
    ag_step(DOWN, 1, L)
    ag_step(DOWN, 1, S)
    finish_rows()
    ag_step(UP, 2, S)
    ag_wait(UP, 2, L)
    ag_step(DOWN, 2, L)
    ag_step(DOWN, 2, S)
    forwarded(DOWN, 0)
    turn_out(5, 7)
    ag_step(DOWN, 3, L)
    ag_wait(UP, 2, S)
    forwarded(DOWN, 1)
    turn_out(4, 5)
    turn_out(7, 8)
    last_send()
    ag_wait(DOWN, 2, S)
    forwarded(DOWN, 2)
    turn_out(2, 4)
    turn_out(8, 10)
    ag_wait(DOWN, 3, L)
    last_wait()
    forwarded(DOWN, 3)
    turn_out(0, 2)
    forwarded(UP)
    last_done()
    wait_bytes(pair_in, pair_send.at[0])
    wait_bytes(send_buf, rs_send.at[0])
    wait_bytes(own_up.at[0 : 13 * share, :], ag_send.at[0])
    wait_bytes(own_up.at[0 : 15 * share, :], fwd_send.at[0])
    wait_bytes(sizes_in, size_send.at[0])
    wait_bytes(rows.at[0, 0 : chips - 1], row_send.at[0])
    wait_bytes(rows.at[0], row_send.at[1])


def put(*refs):
    count = len(refs) // 2
    copies = [pltpu.make_async_copy(refs[i], refs[count + i], refs[-1].at[i]) for i in range(count)]
    for copy in copies:
        copy.start()
    for copy in copies:
        copy.wait()


def shards(chips, models, slope_up, slope_down, slope_norm, param_up, param_down, param_norm):
    size = slope_up.shape[-1]
    share = param_up.shape[0]
    f32, bf16 = jnp.float32, jnp.bfloat16
    hbm = pl.BlockSpec(memory_space=pltpu.HBM)
    vmem = pl.BlockSpec(memory_space=pltpu.VMEM)
    dma = pltpu.SemaphoreType.DMA
    results = (
        jax.ShapeDtypeStruct((size, size), bf16),
        jax.ShapeDtypeStruct((size, size), bf16),
        jax.ShapeDtypeStruct((share, size), f32),
        jax.ShapeDtypeStruct((share, size), f32),
        jax.ShapeDtypeStruct((size,), bf16),
        jax.ShapeDtypeStruct((1, share), f32),
    )
    arrays = (slope_up[0], slope_down[0], slope_norm, param_up, param_down.T, param_norm[None])
    made = pl.pallas_call(
        functools.partial(kernel, size, chips, models),
        name="summed_step",
        out_shape=tuple(pltpu.VMEM(r.shape, r.dtype) for r in results),
        in_specs=[hbm] * 6,
        out_specs=[vmem] * 6,
        scratch_shapes=[
            pltpu.VMEM((size, size), bf16),
            pltpu.VMEM((size, size), bf16),
            pltpu.VMEM((size, size), bf16),
            pltpu.VMEM((2, chips, share, size), bf16),
            pltpu.VMEM((2, 2, 7, share, size // 2), bf16),
            pltpu.VMEM((2, 2, 7, share, size // 2), bf16),
            pltpu.VMEM((size, size), bf16),
            pltpu.VMEM((2, share, size), f32),
            pltpu.VMEM((2, share, size), f32),
            pltpu.VMEM((2, share, 128), f32),
            pltpu.VMEM((2, models - 1, share, 128), f32),
            pltpu.VMEM((2, chips, 1, size + 128), f32),
            pltpu.VMEM((1, size), bf16),
            pltpu.VMEM((1, share), f32),
            dma((10,)),
            dma((1,)),
            dma((2, 5)),
            dma((1,)),
            dma((2, 2, 7)),
            dma((1,)),
            dma((2, 2, 7)),
            dma((1,)),
            dma((6,)),
            dma((1,)),
            dma((2,)),
            dma((2,)),
            dma((8,)),
            dma((4,)),
        ],
        compiler_params=pltpu.CompilerParams(
            collective_id=0, has_side_effects=True, vmem_limit_bytes=48 * 1024 * 1024
        ),
    )(*(pltpu.with_memory_space_constraint(a, pltpu.HBM) for a in arrays))
    half_up, half_down, next_up, next_down, half_norm, next_norm = pl.pallas_call(
        put,
        name="put",
        out_shape=results,
        in_specs=[vmem] * 6,
        out_specs=[hbm] * 6,
        scratch_shapes=[dma((6,))],
        compiler_params=pltpu.CompilerParams(vmem_limit_bytes=1024 * 1024),
    )(*made)
    return (half_up, half_down, half_norm, next_up, next_down.T, next_norm[0])


def solution(mesh):
    chips = mesh.shape["replica"] // 2
    models = mesh.shape["model"]
    return jax.shard_map(
        functools.partial(shards, chips, models),
        mesh=mesh,
        in_specs=(
            P(("copy", "replica"), None, "model"),
            P(("copy", "replica"), "model", None),
            P(("copy", "replica"), None),
            P(("copy", "replica"), "model"),
            P(("copy", "model"), "replica"),
            P(("copy", "replica")),
        ),
        out_specs=(
            P("copy", "model"),
            P(("copy", "model"), None),
            P("copy"),
            P(("copy", "replica"), "model"),
            P(("copy", "model"), "replica"),
            P(("copy", "replica")),
        ),
        check_vma=False,
    )
```

```python
import functools

import jax
import jax.numpy as jnp
from jax import lax
from jax.experimental import pallas as pl
from jax.experimental.pallas import tpu as pltpu
from jax.sharding import PartitionSpec as P

learn_rate = 0.5
eps = 1e-06
MESH = pl.DeviceIdType.MESH
UP, DOWN = 0, 1


def kernel(
    size,
    chips,
    models,
    up_hbm,
    down_hbm,
    norm_hbm,
    param_up_hbm,
    param_down_hbm,
    gain_hbm,
    half_up,
    half_down,
    next_up,
    next_down,
    half_norm,
    next_norm,
    own_up,
    raw_down,
    own_down,
    pair_in,
    send_buf,
    recv_buf,
    gathered,
    param,
    mean,
    sizes,
    sizes_in,
    rows,
    norm_in,
    gain_in,
    load_sem,
    pair_send,
    pair_recv,
    rs_send,
    rs_recv,
    ag_send,
    ag_recv,
    fwd_send,
    fwd_recv,
    size_send,
    size_recv,
    row_send,
    row_recv,
    last_sem,
):
    f32, bf16 = jnp.float32, jnp.bfloat16
    share = size // (2 * chips)
    cols = size // 2
    replica = lax.axis_index("replica")
    model = lax.axis_index("model")
    z, c = replica // 2, replica % 2
    partner = {"replica": z * 2 + (1 - c)}
    rate = (2 * chips) ** (-0.5)

    def chip_at(offset):
        return lax.rem(z + offset + 2 * chips, chips)

    def neighbour(d):
        return {"replica": chip_at(1 if d == 0 else -1) * 2 + c}

    def rows_of(chip, core):
        return pl.ds(pl.multiple_of((chip * 2 + core) * share, 16), share)

    def half_cols(h):
        return pl.ds(h * cols, cols)

    def rdma(src, dst, send, recv, device):
        return pltpu.make_async_remote_copy(
            src_ref=src, dst_ref=dst, send_sem=send, recv_sem=recv, device_id=device, device_id_type=MESH
        )

    own = (own_up, own_down)
    full = (half_up, gathered)
    order = (4, 3, -3, 2, -2, 1, -1, 0)

    def chip_rows(chip):
        return pl.ds(pl.multiple_of(chip * 2 * share, 32), 2 * share)

    def wait_bytes(ref, sem):
        pltpu.make_async_copy(ref, ref, sem).wait()

    def group(o):
        return 4 - abs(o)

    up_loads = {}
    for o in order:
        at = chip_rows(chip_at(o))
        sem = load_sem.at[group(o)]
        up_loads[o] = pltpu.make_async_copy(up_hbm.at[at, :], own_up.at[at, :], sem)
    down_load = pltpu.make_async_copy(down_hbm, raw_down, load_sem.at[5])
    param_loads = [
        pltpu.make_async_copy(param_up_hbm, param.at[UP], load_sem.at[6]),
        pltpu.make_async_copy(param_down_hbm, param.at[DOWN], load_sem.at[7]),
    ]
    row_loads = [
        pltpu.make_async_copy(norm_hbm, norm_in, load_sem.at[8]),
        pltpu.make_async_copy(gain_hbm, gain_in, load_sem.at[9]),
    ]
    for load in [up_loads[4]] + row_loads:
        load.start()

    barrier = pltpu.get_barrier_semaphore()
    others = [partner, neighbour(0), neighbour(1)]
    others += [{"model": lax.rem(model + d, models)} for d in range(1, models)]
    for device in others:
        pl.semaphore_signal(barrier, inc=1, device_id=device, device_id_type=MESH)
    up_loads[3].start()
    up_loads[-3].start()
    up_loads[4].wait()
    for load in [down_load] + [up_loads[o] for o in order[3:]] + param_loads:
        load.start()
    pl.semaphore_wait(barrier, len(others))

    def start_pairs(p, *offsets):
        for o in offsets:
            if p == UP and o in (3, 2, 1, 0):
                wait_bytes(own_up.at[0 : (4 if o else 2) * share, :], load_sem.at[group(o)])
            src = own[p].at[rows_of(chip_at(o), 1 - c), :]
            rdma(src, pair_in.at[p, o % chips], pair_send.at[0], pair_recv.at[p, group(o)], partner).start()

    ready = set()

    def pair_sum(p, o, h):
        if (p, o) == (UP, 4):
            wait_bytes(send_buf.at[0, 0, 0], pair_recv.at[UP, h * 5])
        elif (p, group(o)) not in ready:
            ready.add((p, group(o)))
            wait_bytes(pair_in.at[p, 0 : 1 if o in (4, 0) else 2], pair_recv.at[p, group(o)])
        mine = own[p][rows_of(chip_at(o), c), half_cols(h)]
        return mine.astype(f32) + pair_in[p, o % chips, :, half_cols(h)].astype(f32)

    def rs_index(d, k, h):
        return 0 if k == 0 else 2 * k - 1 + (h != d)

    def rs_copy(p, d, k, h):
        i = rs_index(d, k, h)
        return rdma(send_buf.at[p, d, i], recv_buf.at[p, d, i], rs_send.at[0], rs_recv.at[p, d, i], neighbour(d))

    def rs_step(p, k, long_half):
        for d in range(2):
            h = d if long_half else 1 - d
            value = pair_sum(p, (4 - k if d == 0 else k - 4) if k else 4, h)
            if k >= 2 or (k == 1 and long_half):
                rs_copy(p, d, k - 1, h).wait_recv()
                value = value + recv_buf[p, d, rs_index(d, k - 1, h)].astype(f32)
            send_buf[p, d, rs_index(d, k, h)] = value.astype(bf16)
            rs_copy(p, d, k, h).start()

    def size_copy(p, e):
        return rdma(
            sizes.at[p],
            sizes_in.at[p, e - 1],
            size_send.at[0],
            size_recv.at[p],
            {"model": lax.rem(model + e, models)},
        )

    def finish_sum(p):
        total = jnp.zeros((share, 1), f32)
        for h in range(2):
            for d in range(2):
                rs_copy(p, d, 3, h).wait_recv()
            value = pair_sum(p, 0, h)
            for d in range(2):
                value = value + recv_buf[p, d, rs_index(d, 3, h)].astype(f32)
            value = value * rate
            mean[p, :, half_cols(h)] = value
            total = total + jnp.sum(value * value, axis=1, keepdims=True)
        param_loads[p].wait()
        weights = jnp.sum(param[p] * param[p], axis=1, keepdims=True)
        lane = lax.broadcasted_iota(jnp.int32, (share, 128), 1)
        sizes[p] = jnp.where(lane < 64, total, weights)
        for e in range(1, models):
            size_copy(p, e).start()

    def update(p):
        both = sizes[p]
        wait_bytes(sizes_in.at[p], size_recv.at[p])
        for e in range(1, models):
            both = both + sizes_in[p, e - 1]
        ratio = jnp.sqrt(both[:, 64:65]) * lax.rsqrt(both[:, 0:1] + eps)
        value = param[p] - learn_rate * (mean[p] * ratio)
        out = next_up if p == UP else next_down
        out[...] = value
        full[p][rows_of(z, c), :] = value.astype(bf16)
        at = full[p].at[rows_of(z, c), :]
        rdma(at, at, fwd_send.at[0], fwd_recv.at[forward_group(p, 0)], partner).start()

    def forward_group(p, k, long_half=False):
        return (5 if k == 2 and long_half else 0) if p == UP else k + 1

    def ag_index(d, k, h):
        return 2 * k + (h != d)

    def ag_copy(p, d, k, h, hop):
        chip = chip_at((-k - hop) if d == 0 else (k + hop))
        at = full[p].at[rows_of(chip, c), half_cols(h)]
        i = ag_index(d, k, h)
        return rdma(at, at, ag_send.at[0], ag_recv.at[p, d, i], neighbour(d))

    def forward(p, d, k, h):
        chip = chip_at((-k - 1) if d == 0 else (k + 1))
        at = full[p].at[rows_of(chip, c), half_cols(h)]
        rdma(at, at, fwd_send.at[0], fwd_recv.at[forward_group(p, k, h == d)], partner).start()

    def ag_wait(p, k, long_half, onward=False):
        for d in range(2):
            h = d if long_half else 1 - d
            ag_copy(p, d, k, h, 1).wait_recv()
            forward(p, d, k, h)
            if onward:
                ag_copy(p, d, k + 1, h, 0).start()

    def ag_step(p, k, long_half):
        if k:
            ag_wait(p, k - 1, long_half, True)
        else:
            for d in range(2):
                ag_copy(p, d, k, d if long_half else 1 - d, 0).start()

    def forwarded(p, k=0):
        count = chips - 2 if p == UP else (3, 2, 2, 1)[k]
        wait_bytes(pair_in.at[0, 0:count], fwd_recv.at[forward_group(p, k)])

    def last_rows(d, hop):
        chip = chip_at((-3 - hop) if d == 0 else (3 + hop))
        return full[UP].at[chip_rows(chip), half_cols(d)]

    def last_send():
        @pl.when(c == 1)
        def _():
            wait_bytes(pair_in.at[0, 0:1], fwd_recv.at[5])
            for d in range(2):
                at = last_rows(d, 0)
                rdma(at, at, last_sem.at[0], last_sem.at[1], neighbour(d)).start()

    def last_wait():
        @pl.when(c == 1)
        def _():
            wait_bytes(pair_in.at[0, 0:2], last_sem.at[1])
            for d in range(2):
                at = last_rows(d, 1)
                rdma(at, at, last_sem.at[2], last_sem.at[3], partner).start()

    def last_done():
        @pl.when(c == 1)
        def _():
            wait_bytes(pair_in.at[0, 0:2], last_sem.at[0])
            wait_bytes(pair_in.at[0, 0:2], last_sem.at[2])

        @pl.when(c == 0)
        def _():
            wait_bytes(pair_in.at[0, 0:1], fwd_recv.at[5])
            wait_bytes(pair_in.at[0, 0:2], last_sem.at[3])

    def row_copy(d, k, hop):
        chip = chip_at((-k - hop) if d == 0 else (k + hop))
        at = rows.at[c, chip]
        return rdma(at, at, row_send.at[0], row_recv.at[d * 4 + k], neighbour(d))

    def row_step(k):
        for d in range(2):
            if k:
                if d == 1 and k == 4:
                    continue
                row_copy(d, k - 1, 1).wait_recv()
            if k < 4 - d:
                row_copy(d, k, 0).start()

    def row_pair(core):
        return rdma(rows.at[core], rows.at[core], row_send.at[1], row_recv.at[7], partner)

    def finish_rows():
        row_pair(1 - c).wait_recv()
        total = jnp.zeros((1, size), f32)
        gains = jnp.zeros((8, size), f32)
        wide = lax.broadcasted_iota(jnp.int32, (8, size), 1)
        for chip in range(chips):
            for core in range(2):
                total = total + rows[core, chip, :, :size]
                piece = jnp.broadcast_to(rows[core, chip, :, size:], (8, 128))
                piece = jnp.concatenate([piece] + [jnp.zeros((8, 128), f32)] * (size // 128 - 1), axis=1)
                start = (chip * 2 + core) * share
                moved = pltpu.roll(piece, start, 1) if start else piece
                gains = jnp.where((wide >= start) & (wide < start + share), moved, gains)
        gains = gains - learn_rate * (jnp.broadcast_to(total, (8, size)) * rate)
        half_norm[...] = gains[0].astype(bf16)
        shift = lax.rem(size - replica * share, size)
        next_norm[...] = pltpu.roll(gains, shift, 1)[0:1, 0:share]

    def turn_in(lo, hi):
        @pl.loop(lo, hi)
        def _(i):
            at = pl.ds(pl.multiple_of(i * 128, 128), 128)
            own_down[at, :] = raw_down[:, at].T

    low = (5 * chip_at(4)) // 4

    def turn_out(lo, hi):
        @pl.loop(lo, hi)
        def _(i):
            j = lax.rem(low + i, size // 128)
            at = pl.ds(pl.multiple_of(j * 128, 128), 128)
            half_down[:, at] = gathered[at, :].T

    L, S = True, False
    for h in range(2):
        first = own_up.at[rows_of(chip_at(4), 1 - c), half_cols(h)]
        rdma(first, pair_in.at[UP, 4, :, half_cols(h)], pair_send.at[0], pair_recv.at[UP, h * 5], partner).start()
    for load in row_loads:
        load.wait()
    rows[c, z, :, size:] = jnp.zeros((1, 128), jnp.float32)
    rows[c, z, :, :size] = norm_in[...].astype(jnp.float32)
    rows[c, z, :, size : size + share] = gain_in[...]
    row_step(0)
    rs_step(UP, 0, L)
    start_pairs(UP, 3, -3)
    down_load.wait()
    turn_in(0, size // 128)
    rs_step(UP, 1, S)
    start_pairs(DOWN, 4, 3, -3)
    rs_step(DOWN, 0, L)
    rs_step(DOWN, 1, S)
    start_pairs(UP, 2, -2)
    start_pairs(DOWN, 2, -2)
    rs_step(UP, 1, L)
    start_pairs(UP, 1, -1)
    start_pairs(DOWN, 1, -1)
    start_pairs(UP, 0)
    start_pairs(DOWN, 0)
    rs_step(UP, 2, S)
    rs_step(UP, 2, L)
    rs_step(DOWN, 1, L)
    rs_step(UP, 3, S)
    row_step(1)
    rs_step(UP, 3, L)
    rs_step(DOWN, 2, S)
    rs_step(DOWN, 2, L)
    row_step(2)
    finish_sum(UP)
    rs_step(DOWN, 3, S)
    update(UP)
    ag_step(UP, 0, L)
    rs_step(DOWN, 3, L)
    row_step(3)
    ag_step(UP, 0, S)
    ag_step(UP, 1, L)
    finish_sum(DOWN)
    ag_step(UP, 1, S)
    row_step(4)
    row_pair(c).start()
    update(DOWN)
    ag_step(DOWN, 0, L)
    ag_step(DOWN, 0, S)
    ag_step(UP, 2, L)
    ag_step(DOWN, 1, L)
    ag_step(DOWN, 1, S)
    finish_rows()
    ag_step(UP, 2, S)
    ag_wait(UP, 2, L)
    ag_step(DOWN, 2, L)
    ag_step(DOWN, 2, S)
    forwarded(DOWN, 0)
    turn_out(5, 7)
    ag_step(DOWN, 3, L)
    ag_wait(UP, 2, S)
    forwarded(DOWN, 1)
    turn_out(4, 5)
    turn_out(7, 8)
    last_send()
    ag_wait(DOWN, 2, S)
    forwarded(DOWN, 2)
    turn_out(2, 4)
    turn_out(8, 10)
    ag_wait(DOWN, 3, L)
    last_wait()
    forwarded(DOWN, 3)
    turn_out(0, 2)
    forwarded(UP)
    last_done()
    wait_bytes(pair_in, pair_send.at[0])
    wait_bytes(send_buf, rs_send.at[0])
    wait_bytes(own_up.at[0 : 13 * share, :], ag_send.at[0])
    wait_bytes(own_up.at[0 : 15 * share, :], fwd_send.at[0])
    wait_bytes(sizes_in, size_send.at[0])
    wait_bytes(rows.at[0, 0 : chips - 1], row_send.at[0])
    wait_bytes(rows.at[0], row_send.at[1])


def put(*refs):
    count = len(refs) // 2
    copies = [pltpu.make_async_copy(refs[i], refs[count + i], refs[-1].at[i]) for i in range(count)]
    for copy in copies:
        copy.start()
    for copy in copies:
        copy.wait()


def shards(chips, models, slope_up, slope_down, slope_norm, param_up, param_down, param_norm):
    size = slope_up.shape[-1]
    share = param_up.shape[0]
    f32, bf16 = jnp.float32, jnp.bfloat16
    hbm = pl.BlockSpec(memory_space=pltpu.HBM)
    vmem = pl.BlockSpec(memory_space=pltpu.VMEM)
    dma = pltpu.SemaphoreType.DMA
    results = (
        jax.ShapeDtypeStruct((size, size), bf16),
        jax.ShapeDtypeStruct((size, size), bf16),
        jax.ShapeDtypeStruct((share, size), f32),
        jax.ShapeDtypeStruct((share, size), f32),
        jax.ShapeDtypeStruct((size,), bf16),
        jax.ShapeDtypeStruct((1, share), f32),
    )
    arrays = (slope_up[0], slope_down[0], slope_norm, param_up, param_down.T, param_norm[None])
    made = pl.pallas_call(
        functools.partial(kernel, size, chips, models),
        name="summed_step",
        out_shape=tuple(pltpu.VMEM(r.shape, r.dtype) for r in results),
        in_specs=[hbm] * 6,
        out_specs=[vmem] * 6,
        scratch_shapes=[
            pltpu.VMEM((size, size), bf16),
            pltpu.VMEM((size, size), bf16),
            pltpu.VMEM((size, size), bf16),
            pltpu.VMEM((2, chips, share, size), bf16),
            pltpu.VMEM((2, 2, 7, share, size // 2), bf16),
            pltpu.VMEM((2, 2, 7, share, size // 2), bf16),
            pltpu.VMEM((size, size), bf16),
            pltpu.VMEM((2, share, size), f32),
            pltpu.VMEM((2, share, size), f32),
            pltpu.VMEM((2, share, 128), f32),
            pltpu.VMEM((2, models - 1, share, 128), f32),
            pltpu.VMEM((2, chips, 1, size + 128), f32),
            pltpu.VMEM((1, size), bf16),
            pltpu.VMEM((1, share), f32),
            dma((10,)),
            dma((1,)),
            dma((2, 6)),
            dma((1,)),
            dma((2, 2, 7)),
            dma((1,)),
            dma((2, 2, 7)),
            dma((1,)),
            dma((6,)),
            dma((1,)),
            dma((2,)),
            dma((2,)),
            dma((8,)),
            dma((4,)),
        ],
        compiler_params=pltpu.CompilerParams(
            collective_id=0, has_side_effects=True, vmem_limit_bytes=48 * 1024 * 1024
        ),
    )(*(pltpu.with_memory_space_constraint(a, pltpu.HBM) for a in arrays))
    half_up, half_down, next_up, next_down, half_norm, next_norm = pl.pallas_call(
        put,
        name="put",
        out_shape=results,
        in_specs=[vmem] * 6,
        out_specs=[hbm] * 6,
        scratch_shapes=[dma((6,))],
        compiler_params=pltpu.CompilerParams(vmem_limit_bytes=1024 * 1024),
    )(*made)
    return (half_up, half_down, half_norm, next_up, next_down.T, next_norm[0])


def solution(mesh):
    chips = mesh.shape["replica"] // 2
    models = mesh.shape["model"]
    return jax.shard_map(
        functools.partial(shards, chips, models),
        mesh=mesh,
        in_specs=(
            P(("copy", "replica"), None, "model"),
            P(("copy", "replica"), "model", None),
            P(("copy", "replica"), None),
            P(("copy", "replica"), "model"),
            P(("copy", "model"), "replica"),
            P(("copy", "replica")),
        ),
        out_specs=(
            P("copy", "model"),
            P(("copy", "model"), None),
            P("copy"),
            P(("copy", "replica"), "model"),
            P(("copy", "model"), "replica"),
            P(("copy", "replica")),
        ),
        check_vma=False,
    )
```
